32 devices in a mesh: row: 8 (over y, x, core), col: 4 (over z).
Axes of the slice: x: 2, y: 2, z: 4, core: 2. Of those that a mesh axis runs over, the one named last changes fastest.
Arguments:
- points: float32 [64, 8192], P(None, ('row', 'col')), may hold values from -6 to 6
- labels: int32 [64], P(('row', 'col')), may hold values from 0 to 1
- solution: float32 [8192], P(('row', 'col')), may hold values from -6 to 6
- residual: float32 [8192], P(('row', 'col')), may hold values from -6 to 6
- direction: float32 [8192], P(('row', 'col')), may hold values from -6 to 6
- len_low: float32 [64], replicated, may hold values from 0.75 to 40
- len_high: float32 [64], replicated, may hold values from 0.9 to 40
- variances: float32 [2], replicated, may hold values from 0.5 to 2
- nugget: float32 [2], replicated, may hold values from 0.3 to 1.5
- coupling: float32 [1], replicated, may hold values from 0.6 to 1.6
Outputs:
- solution_next: float32 [8192], P(('row', 'col'))
- residual_next: float32 [8192], P(('row', 'col'))
- direction_next: float32 [8192], P(('row', 'col'))
The draws below stay inside these ranges and needn't reach their ends.
All inputs are finite; a program needn't handle non-finite values.
Results may differ from the reference program's by a relative error of at most 0.00027.
Values sent between devices are 32-bit elements; how exact they have to be, the bound alone decides.
No kernel may reach another device: no remote copies, remote signals or barrier semaphores. Data moves between devices by JAX's collectives and lax.ppermute only.
A program may use at most 64 MiB of HBM per device.

```python
import math
import jax
import jax.numpy as jnp
from jax import lax

FEATURES = 64
NPTS = 8192
BLOCKS = 64


def draw_lengths(key, salt, short_lo, short_hi, long_lo, long_hi):
    ranking = jax.random.permutation(jax.random.fold_in(key, salt + 1), FEATURES)
    relevant = ranking < 6
    first_draw = jax.random.uniform(jax.random.fold_in(key, salt + 2), (FEATURES,), jnp.float32)
    second_draw = jax.random.uniform(jax.random.fold_in(key, salt + 3), (FEATURES,), jnp.float32)
    short_scale = jnp.exp(jnp.log(short_lo) + first_draw * (jnp.log(short_hi) - jnp.log(short_lo)))
    long_scale = jnp.exp(jnp.log(long_lo) + second_draw * (jnp.log(long_hi) - jnp.log(long_lo)))
    return jnp.where(relevant, short_scale, long_scale).astype(jnp.float32)


def draw_len_low(key, part):
    return draw_lengths(key, 100, 0.75, 1.4, 15.0, 40.0)


def draw_len_high(key, part):
    return draw_lengths(key, 200, 0.9, 1.7, 15.0, 40.0)


def draw_points(key, part):
    normals = jax.random.normal(jax.random.fold_in(key, 31), (FEATURES, NPTS), jnp.float32)
    return jnp.clip(normals, -6.0, 6.0).astype(jnp.float32)


def place_ends(drawn, key, low, high):
    place = [jax.random.randint(jax.random.fold_in(key, axis), (), 0, length) for axis, length in enumerate(drawn.shape)]
    widest = drawn.shape.index(max(drawn.shape))
    next_to = place[:widest] + [(place[widest] + 1) % drawn.shape[widest]] + place[widest + 1:]
    return drawn.at[tuple(place)].set(low).at[tuple(next_to)].set(high)


def block_levels(key, extent, split, low, high):
    level, own = 1.0, jax.random.fold_in(key, 6)
    for axis_at, shards_of in split:
        heights = jnp.exp(jax.random.uniform(jax.random.fold_in(own, axis_at), (shards_of,), jnp.float32, low / len(split), high / len(split)))
        level = level * jnp.repeat(heights, extent[axis_at] // shards_of).reshape([-1 if axis == axis_at else 1 for axis in range(len(extent))])
    return level


def noise(key, extent, deviation, reach, split=(), kind=jnp.bfloat16):
    entries = jax.random.normal(key, extent, jnp.float32) * deviation
    if len(split) > 0:
        entries = block_levels(key, extent, split, -0.22, 0.18) * entries
    return jnp.clip(entries, min=-reach, max=reach).astype(kind)


def setup_inputs(seed: int = 0) -> dict:
    splits = jax.random.split(jax.random.key(seed), 11)
    return {
        "points": draw_points(jax.random.fold_in(splits[10], 71), 0),
        "labels": place_ends(jax.random.randint(splits[1], (BLOCKS,), 0, 2), jax.random.fold_in(splits[1], 1), 0, 1).astype(jnp.int32),
        "solution": noise(splits[2], (NPTS,), 1.0, 6.0, ((0, 32),), jnp.float32),
        "residual": noise(splits[3], (NPTS,), 1.0, 6.0, ((0, 32),), jnp.float32),
        "direction": noise(splits[4], (NPTS,), 1.0, 6.0, ((0, 32),), jnp.float32),
        "len_low": draw_len_low(jax.random.fold_in(splits[10], 71), 0),
        "len_high": draw_len_high(jax.random.fold_in(splits[10], 71), 0),
        "variances": jnp.clip(jnp.exp(jax.random.uniform(splits[7], (2,), jnp.float32, math.log(0.5), math.log(2.0))), 0.5, 2.0),
        "nugget": jnp.clip(jnp.exp(jax.random.uniform(splits[8], (2,), jnp.float32, math.log(0.3), math.log(1.5))), 0.3, 1.5),
        "coupling": jnp.clip(jax.random.uniform(splits[9], (1,), jnp.float32, 0.6, 1.6), 0.6, 1.6),
    }


def point_factors(labels, coupling, nugget):
    fidelity = jnp.repeat(labels, 128).astype(jnp.float32)
    row_scale = 1.0 + (coupling[0] - 1.0) * fidelity
    nugget_points = nugget[0] + (nugget[1] - nugget[0]) * fidelity
    return row_scale, fidelity, nugget_points


def reference(points, labels, solution, residual, direction, len_low, len_high, variances, nugget, coupling):
    row_scale, high_mask, nugget_points = point_factors(labels, coupling, nugget)
    low_coords = points / len_low[:, None]
    high_coords = points / len_high[:, None]
    low_norms = jnp.sum(low_coords * low_coords, 0)
    high_norms = jnp.sum(high_coords * high_coords, 0)
    weights_low = row_scale * direction
    weights_high = high_mask * direction
    point_count = points.shape[1]
    row_block = 1024
    numbers = (point_count // row_block)
    dims = (((0,), (0,)), ((), ()))

    def block_rows(block_index):
        offset = block_index * row_block
        block_low = lax.dynamic_slice_in_dim(low_coords, offset, row_block, 1)
        block_high = lax.dynamic_slice_in_dim(high_coords, offset, row_block, 1)
        norm_low = lax.dynamic_slice_in_dim(low_norms, offset, row_block, 0)
        norm_high = lax.dynamic_slice_in_dim(high_norms, offset, row_block, 0)
        dist_low = norm_low[:, None] + low_norms[None, :] - 2.0 * lax.dot_general(
            block_low, low_coords, dims, precision=lax.Precision.HIGHEST)
        dist_high = norm_high[:, None] + high_norms[None, :] - 2.0 * lax.dot_general(
            block_high, high_coords, dims, precision=lax.Precision.HIGHEST)
        sum_low = jnp.dot(jnp.exp(-0.5 * dist_low), weights_low, precision=lax.Precision.HIGHEST)
        sum_high = jnp.dot(jnp.exp(-0.5 * dist_high), weights_high, precision=lax.Precision.HIGHEST)
        return sum_low, sum_high

    sum_low, sum_high = lax.map(block_rows, jnp.arange(numbers, dtype=jnp.int32))
    sum_low = sum_low.reshape(-1)
    sum_high = sum_high.reshape(-1)
    kernel_image = variances[0] * row_scale * sum_low + variances[1] * high_mask * sum_high + nugget_points * direction
    old_norm = jnp.sum(residual * residual)
    curvature = jnp.sum(direction * kernel_image)
    step_size = old_norm / curvature
    solution_next = solution + step_size * direction
    residual_next = residual - step_size * kernel_image
    new_norm = jnp.sum(residual_next * residual_next)
    direction_next = residual_next + (new_norm / old_norm) * direction
    return solution_next, residual_next, direction_next
```

```python
import functools
import math

import jax
import jax.numpy as jnp
from jax import lax
from jax.experimental import pallas as pl
from jax.experimental.pallas import tpu as pltpu
from jax.sharding import PartitionSpec as P


AXES = ("row", "col")
LANES = 128
EXTRA = 8
ROOT = math.sqrt(math.log2(math.e))
VMEM = pl.BlockSpec(memory_space=pltpu.VMEM)
SMEM = pl.BlockSpec(memory_space=pltpu.SMEM)


def partner(index, step, size):
    return index ^ step if size & (size - 1) == 0 else (index - step) % size


def exchange(x, axis, pairs_of, size):
    return lax.ppermute(x, axis, [(pairs_of(i), i) for i in range(size)])


def column(vector):
    n = vector.shape[-1]
    wide = jnp.broadcast_to(vector.reshape(1, n), (n, n))
    here = lax.broadcasted_iota(jnp.int32, (n, n), 0) == lax.broadcasted_iota(jnp.int32, (n, n), 1)
    return jnp.sum(jnp.where(here, wide, 0.0), 1, keepdims=True)


def split(x):
    high = x.astype(jnp.bfloat16)
    return high, (x - high.astype(jnp.float32)).astype(jnp.bfloat16)


def products(
    nrow,
    ncol,
    feats,
    width,
    *refs,
):
    ncols, nrows = nrow, ncol
    col_refs, row_refs = refs[:ncols], refs[ncols : ncols + nrows]
    len_low, len_high, variances, nugget, coupling, out = refs[ncols + nrows : ncols + nrows + 6]
    rhs, brow, wrow, lhs, acol, acc = refs[ncols + nrows + 6 :]
    zone = lax.axis_index("col")
    slope = coupling[0] - 1.0
    inverse = [column(ROOT / ref[...].reshape(1, feats)) for ref in (len_low, len_high)]

    for block, ref in enumerate(col_refs):
        coords = ref[:feats, :]
        direction, label = ref[feats : feats + 1, :], ref[feats + 1 : feats + 2, :]
        for kind in range(2):
            high, mid = split(coords * inverse[kind])
            rhs[kind, block] = jnp.concatenate([high, mid, high, mid], 0)
            kept = high.astype(jnp.float32) + mid.astype(jnp.float32)
            brow[kind, block] = 0.5 * jnp.sum(kept * kept, 0, keepdims=True)
        wrow[0, block] = (1.0 + slope * label) * direction
        wrow[1, block] = label * direction

    for block, ref in enumerate(row_refs):
        coords = ref[:feats, :]
        for kind in range(2):
            scaled = coords * inverse[kind]
            turned = jnp.concatenate([scaled, scaled], 0).T
            high, mid = split(turned)
            lhs[kind, block] = jnp.concatenate([high, mid], 1)
            kept = high.astype(jnp.float32) + mid.astype(jnp.float32)
            norm = 0.25 * jnp.sum(kept * kept, 1, keepdims=True)
            acol[kind, block] = jnp.broadcast_to(norm, (width, LANES))

    acc[...] = jnp.zeros_like(acc)

    def step(block, carry):
        for kind in range(2):
            right, bias, weight = rhs[kind, block], brow[kind, block], wrow[kind, block]
            for at in range(nrows):
                dots = jnp.dot(lhs[kind, at], right, preferred_element_type=jnp.float32)
                shift = acol[kind, at]
                total = acc[kind, at]
                for part in range(width // LANES):
                    lanes = slice(part * LANES, (part + 1) * LANES)
                    total += jnp.exp2(dots[:, lanes] - shift - bias[:, lanes]) * weight[:, lanes]
                acc[kind, at] = total
        return carry

    lax.fori_loop(0, ncols, step, 0)

    pieces = width // LANES
    beta = jnp.zeros((1, LANES), jnp.float32)
    gamma = jnp.zeros((1, LANES), jnp.float32)
    alpha = jnp.zeros((1, LANES), jnp.float32)
    height = nrows * pieces + 1
    for at, ref in enumerate(row_refs):
        place = partner(zone, at, ncol) * pieces if ncol & (ncol - 1) == 0 else lax.rem(zone - at + ncol, ncol) * pieces
        for piece in range(pieces):
            span = slice(piece * LANES, (piece + 1) * LANES)
            low = jnp.sum(acc[0, at, span].T, 0, keepdims=True)
            high = jnp.sum(acc[1, at, span].T, 0, keepdims=True)
            direction, label = ref[feats : feats + 1, span], ref[feats + 1 : feats + 2, span]
            residual = ref[feats + 2 : feats + 3, span]
            image = variances[0] * (1.0 + slope * label) * low + variances[1] * label * high
            if at == 0:
                image += (nugget[0] + (nugget[1] - nugget[0]) * label) * direction
                alpha += residual * residual
            beta += direction * image
            gamma += residual * image
            for peer in range(nrow * ncol):
                out[pl.ds(peer * height + place + piece, 1), :] = image
    lane = lax.broadcasted_iota(jnp.int32, (1, LANES), 1)
    scalars = jnp.where(
        lane == 0, jnp.sum(alpha), jnp.where(lane == 1, jnp.sum(beta), jnp.where(lane == 2, jnp.sum(gamma), 0.0))
    )
    for peer in range(nrow * ncol):
        out[pl.ds(peer * height + height - 1, 1), :] = scalars


def finish(nrow, ncol, pieces, got, solution, residual, direction, out_sol, out_res, out_dir):
    height = ncol * pieces + 1
    mine, zone = lax.axis_index("row"), lax.axis_index("col")
    scalars = jnp.zeros((1, LANES), jnp.float32)
    square = jnp.zeros((ncol * pieces, LANES), jnp.float32)
    for row in range(nrow):
        image = jnp.zeros((ncol * pieces, LANES), jnp.float32)
        for col in range(ncol):
            start = (row * ncol + col) * height
            image += got[start : start + height - 1, :]
            scalars += got[start + height - 1 : start + height, :]
        square += image * image
    lane = lax.broadcasted_iota(jnp.int32, (1, LANES), 1)
    old_norm, curvature, cross = (jnp.sum(jnp.where(lane == n, scalars, 0.0)) for n in range(3))
    image_norm = jnp.sum(square)
    own = jnp.zeros((pieces, LANES), jnp.float32)
    for col in range(ncol):
        own += got[pl.ds((mine * ncol + col) * height + zone * pieces, pieces), :]
    step = jnp.full((1, LANES), old_norm) / jnp.full((1, LANES), curvature)
    new_norm = old_norm - 2.0 * step * cross + step * step * image_norm
    out_sol[...] = solution[...] + step * direction[...]
    after = residual[...] - step * own
    out_res[...] = after
    out_dir[...] = after + new_norm / jnp.full((1, LANES), old_norm) * direction[...]


def body(
    nrow, ncol, points, labels, solution, residual, direction, len_low, len_high, variances, nugget, coupling
):
    feats, width = points.shape
    pieces = width // LANES
    label = jnp.repeat(labels, width // labels.shape[0]).astype(jnp.float32)
    own = jnp.concatenate(
        [
            points,
            direction[None],
            label[None],
            residual[None],
            jnp.zeros((EXTRA - 3, width), jnp.float32),
        ],
        0,
    )
    rows = [own] + [
        exchange(own, "col", lambda i, s=s: partner(i, s, ncol), ncol) for s in range(1, ncol)
    ]
    cores = 2 if nrow % 2 == 0 else 1
    chips = nrow // cores
    cols = [own] + [
        exchange(own, "row", lambda i, s=s: partner(i // cores, s, chips) * cores + i % cores, nrow)
        for s in range(1, chips)
    ]
    if cores == 2:
        cols += [exchange(block, "row", lambda i: i ^ 1, nrow) for block in cols]
    height = ncol * pieces + 1
    devices = nrow * ncol
    sent = pl.pallas_call(
        functools.partial(products, nrow, ncol, feats, width),
        out_shape=jax.ShapeDtypeStruct((devices * height, LANES), jnp.float32),
        in_specs=[VMEM] * (nrow + ncol + 2) + [SMEM] * 3,
        out_specs=VMEM,
        scratch_shapes=[
            pltpu.VMEM((2, nrow, 4 * feats, width), jnp.bfloat16),
            pltpu.VMEM((2, nrow, 1, width), jnp.float32),
            pltpu.VMEM((2, nrow, 1, width), jnp.float32),
            pltpu.VMEM((2, ncol, width, 4 * feats), jnp.bfloat16),
            pltpu.VMEM((2, ncol, width, LANES), jnp.float32),
            pltpu.VMEM((2, ncol, width, LANES), jnp.float32),
        ],
        name="products",
    )(*cols, *rows, len_low.reshape(1, feats), len_high.reshape(1, feats), variances, nugget, coupling)
    got = lax.all_to_all(sent.reshape(devices, 1, height * LANES), AXES, 0, 0)
    flat = [x.reshape(pieces, LANES) for x in (solution, residual, direction)]
    outs = pl.pallas_call(
        functools.partial(finish, nrow, ncol, pieces),
        out_shape=[jax.ShapeDtypeStruct((pieces, LANES), jnp.float32)] * 3,
        in_specs=[VMEM] * 4,
        out_specs=[VMEM] * 3,
        name="finish",
    )(got.reshape(devices * height, LANES), *flat)
    return tuple(x.reshape(width) for x in outs)


def solution(mesh):
    split_points = P(AXES)
    placed = (P(None, AXES),) + (split_points,) * 4 + (P(),) * 5
    return jax.shard_map(
        functools.partial(body, mesh.shape["row"], mesh.shape["col"]),
        mesh=mesh,
        in_specs=placed,
        out_specs=(split_points,) * 3,
        check_vma=False,
    )
```
